128 devices in a mesh: dp: 1, sp: 128 (over z, y, x, core).
Axes of the slice: x: 4, y: 4, z: 4, core: 2. Of those that a mesh axis runs over, the one named last changes fastest.
Arguments:
- patches: bfloat16 [4, 65536, 1024], P('dp', 'sp')
- ln1_scale: float32 [1024], replicated
- ln1_bias: float32 [1024], replicated
- w_tok1: bfloat16 [65536, 512], replicated
- b_tok1: float32 [512], replicated
- w_tok2: bfloat16 [512, 65536], replicated
- b_tok2: float32 [65536], replicated
- ln2_scale: float32 [1024], replicated
- ln2_bias: float32 [1024], replicated
- w_ch1: bfloat16 [1024, 4096], replicated
- b_ch1: float32 [4096], replicated
- w_ch2: bfloat16 [4096, 1024], replicated
- b_ch2: float32 [1024], replicated
Outputs:
- output: bfloat16 [4, 65536, 1024], P('dp', 'sp')
All inputs are finite; a program needn't handle non-finite values.
Results may differ from the reference program's by a relative error of at most 0.0111779.
Values are sent between devices in bfloat16 or wider.
A program may use at most 1 GiB of HBM per device.

```python
import jax
import jax.numpy as jnp
from jax import lax

BATCH = 4
SEQ_DEV = 512
GROUP = 128
CHANNELS = 1024
TOK_HIDDEN = 512
CH_HIDDEN = 4096
SEQ_LEN = SEQ_DEV * GROUP
LN_EPS = 1e-6


def layer_norm(rows, scale, offset):
    rows_wide = rows.astype(jnp.float32)
    row_mean = jnp.mean(rows_wide, axis=-1, keepdims=True)
    centered = rows_wide - row_mean
    row_var = jnp.mean(centered * centered, axis=-1, keepdims=True)
    return (centered * lax.rsqrt(row_var + LN_EPS) * scale + offset).astype(jnp.bfloat16)


def setup_inputs(seed: int = 0, part: int = 0) -> dict:
    keys = jax.random.split(jax.random.key(seed), 13)

    def draw_normal(index, shape):
        return jax.random.normal(keys[index], shape, jnp.float32)

    patches = jax.random.normal(jax.random.fold_in(keys[0], part), (BATCH, SEQ_LEN, CHANNELS), jnp.float32)
    return dict(
        patches=patches.astype(jnp.bfloat16),
        ln1_scale=1.0 + 0.3 * draw_normal(1, (CHANNELS,)),
        ln1_bias=0.3 * draw_normal(2, (CHANNELS,)),
        w_tok1=(draw_normal(3, (SEQ_LEN, TOK_HIDDEN)) * SEQ_LEN ** -0.5).astype(jnp.bfloat16),
        b_tok1=0.5 * draw_normal(4, (TOK_HIDDEN,)),
        w_tok2=(draw_normal(5, (TOK_HIDDEN, SEQ_LEN)) * TOK_HIDDEN ** -0.5).astype(jnp.bfloat16),
        b_tok2=0.5 * draw_normal(6, (SEQ_LEN,)),
        ln2_scale=1.0 + 0.3 * draw_normal(7, (CHANNELS,)),
        ln2_bias=0.3 * draw_normal(8, (CHANNELS,)),
        w_ch1=(draw_normal(9, (CHANNELS, CH_HIDDEN)) * CHANNELS ** -0.5).astype(jnp.bfloat16),
        b_ch1=0.5 * draw_normal(10, (CH_HIDDEN,)),
        w_ch2=(draw_normal(11, (CH_HIDDEN, CHANNELS)) * CH_HIDDEN ** -0.5).astype(jnp.bfloat16),
        b_ch2=0.5 * draw_normal(12, (CHANNELS,)),
    )


def reference(patches, ln1_scale, ln1_bias, w_tok1, b_tok1, w_tok2, b_tok2, ln2_scale, ln2_bias, w_ch1, b_ch1, w_ch2, b_ch2):
    w_tok2_blocks = jnp.transpose(w_tok2.reshape(TOK_HIDDEN, GROUP, SEQ_DEV), (1, 0, 2))
    b_tok2_blocks = b_tok2.reshape(GROUP, SEQ_DEV)

    def one_image(image):
        normed = layer_norm(image, ln1_scale, ln1_bias)
        hidden = jnp.dot(w_tok1.T, normed, preferred_element_type=jnp.float32) + b_tok1[:, None]
        act_tok = jax.nn.gelu(hidden, approximate=True).astype(jnp.bfloat16)
        image_blocks = image.reshape(GROUP, SEQ_DEV, CHANNELS)

        def one_block(block_args):
            rows, w_rows, b_rows = block_args
            mixed = (jnp.dot(w_rows.T, act_tok, preferred_element_type=jnp.float32) + b_rows[:, None]).astype(jnp.bfloat16)
            residual = (rows.astype(jnp.float32) + mixed.astype(jnp.float32)).astype(jnp.bfloat16)
            chan_in = layer_norm(residual, ln2_scale, ln2_bias)
            pre_act = jnp.dot(chan_in, w_ch1, preferred_element_type=jnp.float32) + b_ch1
            act_ch = jax.nn.gelu(pre_act, approximate=True).astype(jnp.bfloat16)
            ch_out = jnp.dot(act_ch, w_ch2, preferred_element_type=jnp.float32) + b_ch2
            return (residual.astype(jnp.float32) + ch_out).astype(jnp.bfloat16)

        out_blocks = lax.map(one_block, (image_blocks, w_tok2_blocks, b_tok2_blocks))
        return out_blocks.reshape(SEQ_LEN, CHANNELS)

    return lax.map(one_image, patches)
```

```python
import functools
import math

import jax
import jax.numpy as jnp
from jax import lax
from jax.experimental import pallas as pl
from jax.experimental.pallas import tpu as pltpu
from jax.sharding import PartitionSpec as P

LN_EPS = 1e-6
IMAGES = 4
ROWS = 512
CH = 1024
TOK = 512
HID = 4096
RING = 4
LANES = 128
UNITS = CH // 2 // LANES
BLOCK = (128, 32, 8)
E_TILE = 512
N_SLOTS = HID // E_TILE
F32 = jnp.float32
BF16 = jnp.bfloat16

GELU_A = math.sqrt(2.0 / math.pi)
GELU_B = GELU_A * 0.044715


def gelu(a):
    return (0.5 * a) * (1.0 + jnp.tanh(a * (GELU_A + GELU_B * (a * a))))


def layer_norm(rows, scale, offset):
    wide = rows.astype(F32)
    mean = jnp.mean(wide, axis=-1, keepdims=True)
    centered = wide - mean
    var = jnp.mean(centered * centered, axis=-1, keepdims=True)
    return (centered * lax.rsqrt(var + LN_EPS) * scale + offset).astype(BF16)


def layer_kernel(
    x_hbm, w_tok1_hbm, w_tok2_hbm, w_ch1_hbm, w_ch2_hbm,
    ln1_s, ln1_b, b_tok1, b_tok2, ln2_s, ln2_b, b_ch1, b_ch2,
    out_hbm,
    xv, w1raw, w2raw, w1t, w2t, wc1, wc2, b1col, b2col,
    usend, upair, part, got0, got1, got2, sum1, sum2, g, v, acc,
    load_sem, store_sem, u_send, u_recv, rs_send, rs_recv, ag_send, ag_recv, d_send, d_recv,
):
    me = lax.axis_index('sp')
    core = me % 2
    chip = me // 2
    partner = chip * 2 + (1 - core)

    def at(index):
        return {'sp': index}

    def geometry(b, q):
        color = (q + core + b) % 3
        places, strides = [], []
        for p in range(3):
            axis = (color + p) % 3
            stride = 1 + (3 * axis * (3 * axis - 1)) // 2
            strides.append(stride)
            places.append((chip // stride) % RING)
        return places, strides

    def peer(place, stride, j):
        other = (place + j) % RING
        return other, (chip + (other - place) * stride) * 2 + core

    loads = []

    def load(n, src, dst):
        c = pltpu.make_async_copy(src, dst, load_sem.at[n])
        c.start()
        loads.append(c)

    load(0, x_hbm.at[0], xv.at[0])
    load(1, w_tok1_hbm.at[pl.ds(pl.multiple_of(chip * (2 * ROWS), 2 * ROWS), 2 * ROWS)], w1raw)
    for b in range(1, IMAGES):
        load(1 + b, x_hbm.at[b], xv.at[b])
    load(5, w_tok2_hbm.at[:, pl.ds(pl.multiple_of(me * ROWS, ROWS), ROWS)], w2raw)
    load(6, w_ch1_hbm, wc1)
    load(7, w_ch2_hbm, wc2)

    barrier = pltpu.get_barrier_semaphore()
    pl.semaphore_signal(barrier, inc=1, device_id=at(partner), device_id_type=pl.DeviceIdType.MESH)
    for stride in (1, 4, 16):
        place = (chip // stride) % RING
        for j in range(1, RING):
            _, other = peer(place, stride, j)
            pl.semaphore_signal(barrier, inc=1, device_id=at(other), device_id_type=pl.DeviceIdType.MESH)

    def remote(src, dst, send, recv, device):
        return pltpu.make_async_remote_copy(
            src_ref=src, dst_ref=dst, send_sem=send, recv_sem=recv,
            device_id=at(device), device_id_type=pl.DeviceIdType.MESH)

    def arrived(ref, sem):
        pltpu.make_async_copy(ref, ref, sem).wait()

    def norm1(b):
        def chunk(i, _):
            rows = pl.ds(pl.multiple_of(i * 128, 128), 128)
            u = layer_norm(xv[b, rows, :], ln1_s[...], ln1_b[...])
            mine = pl.ds(pl.multiple_of(core * ROWS + i * 128, 128), 128)

            @pl.when(core == 0)
            def _():
                upair[b, mine, :] = u[:, :CH // 2]
                usend[b, rows, :] = u[:, CH // 2:]

            @pl.when(core == 1)
            def _():
                upair[b, mine, :] = u[:, CH // 2:]
                usend[b, rows, :] = u[:, :CH // 2]
            return 0
        lax.fori_loop(0, ROWS // 128, chunk, 0)

    def my_rows():
        return pl.ds(pl.multiple_of(core * ROWS, ROWS), ROWS)

    def send_u(b):
        remote(usend.at[b], upair.at[b, my_rows()], u_send.at[b], u_recv.at[b], partner).start()

    def hidden(b):
        arrived(usend.at[b], u_recv.at[b])

        def unit(i, _):
            cols = pl.ds(pl.multiple_of(i * 256, 256), 256)
            h = jnp.dot(w1t[...], upair[b, :, cols], preferred_element_type=F32)
            part[b, 2 * i] = h[:, :LANES]
            part[b, 2 * i + 1] = h[:, LANES:]
            return 0
        lax.fori_loop(0, 2, unit, 0)

    def blk(place, size):
        return pl.ds(pl.multiple_of(place * size, size), size)

    def scatter_start(b, p):
        src = (part, sum1, sum2)[p]
        dst = (got0, got1, got2)[p]

        def unit(q, _):
            places, strides = geometry(b, q)
            for j in range(1, RING):
                place, device = peer(places[p], strides[p], j)
                remote(src.at[b, q, blk(place, BLOCK[p])], dst.at[b, q, j - 1],
                       rs_send.at[b, p], rs_recv.at[b, p, q], device).start()
            return 0
        lax.fori_loop(0, UNITS, unit, 0)

    def scatter_add(b, p):
        src = (part, sum1, sum2)[p]
        got = (got0, got1, got2)[p]

        def unit(q, _):
            places, _ = geometry(b, q)
            arrived(got.at[b, q], rs_recv.at[b, p, q])
            total = src[b, q, blk(places[p], BLOCK[p]), :] + got[b, q, 0]
            total = total + got[b, q, 1]
            total = total + got[b, q, 2]
            if p < 2:
                (sum1, sum2)[p][b, q] = total
            else:
                base = places[0] * 128 + places[1] * 32 + places[2] * 8
                h = total + b1col[blk(base // 8, 8), :]
                g[b, core * UNITS + q, base // 8] = gelu(h).astype(BF16)
            return 0
        lax.fori_loop(0, UNITS, unit, 0)

    def owned(b, q, p, places):
        base = places[0] * 16
        if p >= 1:
            base = base + places[1] * 4
        if p >= 2:
            base = base + places[2]
        n = BLOCK[p] // 8
        return g.at[b, core * UNITS + q, blk(base // n, n)]

    def gather_start(b, p):
        def unit(q, _):
            places, strides = geometry(b, q)
            mine = owned(b, q, p, places)
            for j in range(1, RING):
                _, device = peer(places[p], strides[p], j)
                remote(mine, mine, ag_send.at[b, p], ag_recv.at[b, p, q], device).start()
            return 0
        lax.fori_loop(0, UNITS, unit, 0)

    def gather_wait(b, p):
        n = 3 * BLOCK[p] // 8

        def unit(q, _):
            arrived(g.at[b, core * UNITS + q, pl.ds(0, n)], ag_recv.at[b, p, q])
            return 0
        lax.fori_loop(0, UNITS, unit, 0)

    def swap_start(b):
        def unit(q, _):
            mine = g.at[b, core * UNITS + q]
            remote(mine, mine, d_send.at[b], d_recv.at[b, q], partner).start()
            return 0
        lax.fori_loop(0, UNITS, unit, 0)

    def swap_wait(b):
        def unit(q, _):
            arrived(g.at[b, (1 - core) * UNITS + q], d_recv.at[b, q])
            return 0
        lax.fori_loop(0, UNITS, unit, 0)

    def step(b, k):
        if k == 0:
            scatter_start(b, 0)
        elif k in (1, 2):
            scatter_add(b, k - 1)
            scatter_start(b, k)
        elif k == 3:
            scatter_add(b, 2)
            gather_start(b, 2)
        elif k in (4, 5):
            gather_wait(b, 6 - k)
            gather_start(b, 5 - k)
        elif k == 6:
            gather_wait(b, 0)
            swap_start(b)
        else:
            swap_wait(b)

    def token_mix(b):
        def pair(i, _):
            left = g[b, 2 * i].reshape(TOK, LANES)
            right = g[b, 2 * i + 1].reshape(TOK, LANES)
            t = jnp.dot(w2t[...], jnp.concatenate([left, right], axis=1), preferred_element_type=F32)
            bias = b2col[...]
            t = (t + jnp.concatenate([bias, bias], axis=1)).astype(BF16)
            cols = pl.ds(pl.multiple_of(i * 256, 256), 256)
            xv[b, :, cols] = (xv[b, :, cols].astype(F32) + t.astype(F32)).astype(BF16)
            return 0
        lax.fori_loop(0, CH // 256, pair, 0)

    def norm2(b):
        def chunk(i, _):
            rows = pl.ds(pl.multiple_of(i * 128, 128), 128)
            v[rows, :] = layer_norm(xv[b, rows, :], ln2_s[...], ln2_b[...])
            return 0
        lax.fori_loop(0, ROWS // 128, chunk, 0)

    def channel_mix(b, steps):
        acc[...] = jnp.zeros_like(acc)

        def slot(j, _):
            e = pl.ds(pl.multiple_of(j * E_TILE, E_TILE), E_TILE)
            pre = jnp.dot(v[...], wc1[:, e], preferred_element_type=F32) + b_ch1[:, e]
            act = gelu(pre).astype(BF16)
            acc[...] += jnp.dot(act, wc2[e, :], preferred_element_type=F32)
            for when, image, k in steps:
                @pl.when(j == when)
                def _():
                    step(image, k)
            return 0
        lax.fori_loop(0, N_SLOTS, slot, 0)

        def chunk(i, _):
            rows = pl.ds(pl.multiple_of(i * 64, 64), 64)
            xv[b, rows, :] = (xv[b, rows, :].astype(F32) + (acc[rows, :] + b_ch2[...])).astype(BF16)
            return 0
        lax.fori_loop(0, ROWS // 64, chunk, 0)
        pltpu.make_async_copy(xv.at[b], out_hbm.at[b], store_sem.at[b]).start()

    loads[0].wait()
    norm1(0)
    pl.semaphore_wait(barrier, 1 + 3 * (RING - 1))
    send_u(0)
    loads[1].wait()
    for i in range(4):
        rows = pl.ds(i * 256, 256)
        w1t[:, rows] = w1raw[rows, :].T
    for m in range(4):
        row = b_tok1[m:m + 1, :]
        b1col[m * LANES:(m + 1) * LANES, :] = jnp.broadcast_to(row, (LANES, LANES)).T
    hidden(0)
    step(0, 0)
    loads[2].wait()
    norm1(1)
    send_u(1)
    for m in range(4):
        row = b_tok2[pl.ds(me * 4 + m, 1), :]
        b2col[m * LANES:(m + 1) * LANES, :] = jnp.broadcast_to(row, (LANES, LANES)).T
    hidden(1)
    step(0, 1)
    step(1, 0)
    loads[3].wait()
    norm1(2)
    send_u(2)
    step(0, 2)
    loads[5].wait()
    for i in range(2):
        cols = pl.ds(i * 256, 256)
        w2t[cols, :] = w2raw[:, cols].T
    hidden(2)
    step(1, 1)
    step(0, 3)
    loads[4].wait()
    norm1(3)
    send_u(3)
    step(1, 2)
    step(0, 4)
    hidden(3)
    step(2, 0)
    step(0, 5)
    step(1, 3)
    step(0, 6)
    step(1, 4)
    step(3, 0)
    step(0, 7)
    loads[6].wait()
    loads[7].wait()

    plan = {
        0: [(0, 1, 5), (2, 2, 1), (3, 1, 6), (4, 2, 2), (5, 3, 1), (6, 2, 3), (7, 1, 7)],
        1: [(0, 3, 2), (1, 2, 4), (2, 3, 3), (3, 2, 5), (4, 3, 4), (5, 2, 6), (6, 3, 5), (7, 2, 7)],
        2: [(1, 3, 6), (5, 3, 7)],
        3: [],
    }
    for b in range(IMAGES):
        token_mix(b)
        norm2(b)
        channel_mix(b, plan[b])

    for b in range(IMAGES):
        arrived(usend.at[b], u_send.at[b])
        for p, got in enumerate((got0, got1, got2)):
            arrived(got.at[b], rs_send.at[b, p])
            arrived(g.at[b, pl.ds(0, UNITS), pl.ds(0, 3 * BLOCK[p] // 8)], ag_send.at[b, p])
        arrived(g.at[b, pl.ds(0, UNITS)], d_send.at[b])
        pltpu.make_async_copy(xv.at[b], out_hbm.at[b], store_sem.at[b]).wait()


def solution(mesh):
    row_spec = P('dp', 'sp', None)
    full_spec = P()

    def local_layer(patches, ln1_scale, ln1_bias, w_tok1, b_tok1, w_tok2, b_tok2, ln2_scale, ln2_bias, w_ch1, b_ch1, w_ch2, b_ch2):
        vmem = pl.BlockSpec(memory_space=pltpu.VMEM)
        hbm = pl.BlockSpec(memory_space=pl.ANY)
        dma = pltpu.SemaphoreType.DMA
        call = pl.pallas_call(
            layer_kernel,
            name='mixer_layer',
            out_shape=jax.ShapeDtypeStruct(patches.shape, BF16),
            in_specs=[hbm] * 5 + [vmem] * 8,
            out_specs=hbm,
            scratch_shapes=[
                pltpu.VMEM((IMAGES, ROWS, CH), BF16),
                pltpu.VMEM((2 * ROWS, TOK), BF16),
                pltpu.VMEM((TOK, ROWS), BF16),
                pltpu.VMEM((TOK, 2 * ROWS), BF16),
                pltpu.VMEM((ROWS, TOK), BF16),
                pltpu.VMEM((CH, HID), BF16),
                pltpu.VMEM((HID, CH), BF16),
                pltpu.VMEM((TOK, LANES), F32),
                pltpu.VMEM((ROWS, LANES), F32),
                pltpu.VMEM((IMAGES, ROWS, CH // 2), BF16),
                pltpu.VMEM((IMAGES, 2 * ROWS, CH // 2), BF16),
                pltpu.VMEM((IMAGES, UNITS, TOK, LANES), F32),
                pltpu.VMEM((IMAGES, UNITS, 3, BLOCK[0], LANES), F32),
                pltpu.VMEM((IMAGES, UNITS, 3, BLOCK[1], LANES), F32),
                pltpu.VMEM((IMAGES, UNITS, 3, BLOCK[2], LANES), F32),
                pltpu.VMEM((IMAGES, UNITS, BLOCK[0], LANES), F32),
                pltpu.VMEM((IMAGES, UNITS, BLOCK[1], LANES), F32),
                pltpu.VMEM((IMAGES, 2 * UNITS, TOK // 8, 8, LANES), BF16),
                pltpu.VMEM((ROWS, CH), BF16),
                pltpu.VMEM((ROWS, CH), F32),
                dma((8,)), dma((IMAGES,)),
                dma((IMAGES,)), dma((IMAGES,)),
                dma((IMAGES, 3)), dma((IMAGES, 3, UNITS)),
                dma((IMAGES, 3)), dma((IMAGES, 3, UNITS)),
                dma((IMAGES,)), dma((IMAGES, UNITS)),
            ],
            compiler_params=pltpu.CompilerParams(
                collective_id=0, has_side_effects=True, vmem_limit_bytes=64 * 1024 * 1024 - 65536),
        )
        return call(
            patches, w_tok1, w_tok2, w_ch1, w_ch2,
            ln1_scale.reshape(1, CH), ln1_bias.reshape(1, CH),
            b_tok1.reshape(TOK // LANES, LANES), b_tok2.reshape(-1, LANES),
            ln2_scale.reshape(1, CH), ln2_bias.reshape(1, CH),
            b_ch1.reshape(1, HID), b_ch2.reshape(1, CH))

    return jax.shard_map(local_layer, mesh=mesh, in_specs=(row_spec,) + (full_spec,) * 12, out_specs=row_spec, check_vma=False)
```

```python
import functools
import math

import jax
import jax.numpy as jnp
from jax import lax
from jax.experimental import pallas as pl
from jax.experimental.pallas import tpu as pltpu
from jax.sharding import PartitionSpec as P

LN_EPS = 1e-6
IMAGES = 4
ROWS = 512
CH = 1024
TOK = 512
HID = 4096
RING = 4
DEVICES = 2 * RING ** 3
LANES = 128
UNITS = CH // 2 // LANES
BLOCK = (128, 32, 8)
NORM_ROWS = 128
ALL = (0, UNITS)
FILL = (
    (0, 1, ALL), (1, 0, (0, 2)), (0, 2, ALL), (1, 0, (2, 4)), (0, 3, ALL), (0, 4, ALL), (1, 1, ALL),
    (0, 5, ALL), (1, 2, ALL), (0, 6, ALL), (1, 3, ALL), (0, 7, ALL), (2, 0, ALL),
)
PLAN = {
    (0, 1): [(1, 4)], (0, 2): [(1, 5), (2, 1)], (0, 3): [(1, 6), (2, 2), (3, 0)],
    (1, 0): [(1, 7)], (1, 1): [(2, 3), (3, 1)], (1, 2): [(2, 4), (3, 2)], (1, 3): [(2, 5), (3, 3)],
    (2, 0): [(2, 6), (3, 4), (2, 7)], (2, 1): [(3, 5)], (2, 3): [(3, 6)],
}
F32 = jnp.float32
BF16 = jnp.bfloat16

GELU_A = math.sqrt(2.0 / math.pi)
GELU_B = GELU_A * 0.044715


def gelu(a):
    return (0.5 * a) * (1.0 + jnp.tanh(a * (GELU_A + GELU_B * (a * a))))


def layer_norm(rows, scale, offset):
    wide = rows.astype(F32)
    mean = jnp.mean(wide, axis=-1, keepdims=True)
    centered = wide - mean
    var = jnp.mean(centered * centered, axis=-1, keepdims=True)
    return (centered * lax.rsqrt(var + LN_EPS) * scale + offset).astype(BF16)


def layer_kernel(
    x_hbm, w_tok1_hbm, w_tok2_hbm, w_ch1_hbm, w_ch2_hbm,
    *rest,
):
    small, (out_hbm, *rest) = rest[:8], rest[8:]
    (
    ln1_s, ln1_b, b_tok1, b_tok2, ln2_s, ln2_b, b_ch1, b_ch2,
    xv, w1raw, w2raw, w1t, w2t, wc1, wc2, b1col, b2col,
    u, upeer, part, got0, got1, got2, sum1, sum2, g, v, acc,
    load_sem, store_sem, u_send, u_recv, rs_send, rs_recv, ag_send, ag_recv, d_send, d_recv,
    ) = rest
    me = lax.axis_index('sp')
    core = me % 2
    chip = me // 2
    partner = chip * 2 + (1 - core)

    def at(index):
        return {'sp': index}

    def geometry(b, q):
        color = (q + core + b) % 3
        places, strides = [], []
        for p in range(3):
            axis = (color + p) % 3
            stride = 1 + (3 * axis * (3 * axis - 1)) // 2
            strides.append(stride)
            places.append((chip // stride) % RING)
        return places, strides

    def peer(place, stride, j):
        other = (place + j) % RING
        return other, (chip + (other - place) * stride) * 2 + core

    loads = []

    def load(n, src, dst):
        c = pltpu.make_async_copy(src, dst, load_sem.at[n])
        c.start()
        loads.append(c)

    load(0, x_hbm.at[0], xv.at[0])
    small_vmem = (ln1_s, ln1_b, b_tok1, b_tok2, ln2_s, ln2_b, b_ch1, b_ch2)
    small_loads = [pltpu.make_async_copy(s, d, load_sem.at[8 + n]) for n, (s, d) in enumerate(zip(small, small_vmem))]
    for c in small_loads:
        c.start()
    load(1, w_tok1_hbm.at[pl.ds(pl.multiple_of(chip * (2 * ROWS), 2 * ROWS), 2 * ROWS)], w1raw)

    barrier = pltpu.get_barrier_semaphore()
    pl.semaphore_signal(barrier, inc=1, device_id=at(partner), device_id_type=pl.DeviceIdType.MESH)
    for stride in (1, 4, 16):
        place = (chip // stride) % RING
        for j in range(1, RING):
            _, other = peer(place, stride, j)
            pl.semaphore_signal(barrier, inc=1, device_id=at(other), device_id_type=pl.DeviceIdType.MESH)

    def remote(src, dst, send, recv, device):
        return pltpu.make_async_remote_copy(
            src_ref=src, dst_ref=dst, send_sem=send, recv_sem=recv,
            device_id=at(device), device_id_type=pl.DeviceIdType.MESH)

    def arrived(ref, sem):
        pltpu.make_async_copy(ref, ref, sem).wait()

    half = CH // 2
    mine = pl.ds(pl.multiple_of(core * half, half), half)
    theirs = pl.ds(pl.multiple_of((1 - core) * half, half), half)

    def norm1(b):
        for i in range(ROWS // NORM_ROWS):
            rows = pl.ds(i * NORM_ROWS, NORM_ROWS)
            u[b, rows, :] = layer_norm(xv[b, rows, :], ln1_s[...], ln1_b[...])

    def send_u(b):
        remote(u.at[b, :, theirs], upeer.at[b], u_send.at[b], u_recv.at[b], partner).start()

    def hidden(b):
        arrived(upeer.at[b], u_recv.at[b])
        own = w1t[:, pl.ds(pl.multiple_of(core * ROWS, ROWS), ROWS)]
        other = w1t[:, pl.ds(pl.multiple_of((1 - core) * ROWS, ROWS), ROWS)]
        for i in range(2):
            cols = pl.ds(pl.multiple_of(core * half + i * 256, 256), 256)
            h = (jnp.dot(own, u[b, :, cols], preferred_element_type=F32)
                 + jnp.dot(other, upeer[b, :, i * 256:(i + 1) * 256], preferred_element_type=F32))
            part[b, 2 * i] = h[:, :LANES]
            part[b, 2 * i + 1] = h[:, LANES:]
            if b == 0:
                step(0, 0, (2 * i, 2 * i + 2))

    def blk(place, size):
        return pl.ds(pl.multiple_of(place * size, size), size)

    def scatter_start(b, p, q):
        src = (part, sum1, sum2)[p]
        dst = (got0, got1, got2)[p]
        places, strides = geometry(b, q)
        for j in (2, 1, 3):
            place, device = peer(places[p], strides[p], j)
            remote(src.at[b, q, blk(place, BLOCK[p])], dst.at[b, q, j - 1],
                   rs_send.at[b, p], rs_recv.at[b, p, q], device).start()

    def scatter_add(b, p, q):
        src = (part, sum1, sum2)[p]
        got = (got0, got1, got2)[p]
        places, _ = geometry(b, q)
        arrived(got.at[b, q], rs_recv.at[b, p, q])
        total = src[b, q, blk(places[p], BLOCK[p]), :] + got[b, q, 0]
        total = total + got[b, q, 1]
        total = total + got[b, q, 2]
        if p < 2:
            (sum1, sum2)[p][b, q] = total
        else:
            base = places[0] * 128 + places[1] * 32 + places[2] * 8
            h = total + b1col[blk(base // 8, 8), :]
            g[b, core * UNITS + q, base // 8] = gelu(h).astype(BF16)

    def owned(b, q, p, places):
        base = places[0] * 16
        if p >= 1:
            base = base + places[1] * 4
        if p >= 2:
            base = base + places[2]
        n = BLOCK[p] // 8
        return g.at[b, core * UNITS + q, blk(base // n, n)]

    def gather_start(b, p, q):
        places, strides = geometry(b, q)
        piece = owned(b, q, p, places)
        for j in (2, 1, 3):
            _, device = peer(places[p], strides[p], j)
            remote(piece, piece, ag_send.at[b, p], ag_recv.at[b, p, q], device).start()

    def gather_wait(b, p, q):
        arrived(g.at[b, core * UNITS + q, pl.ds(0, 3 * BLOCK[p] // 8)], ag_recv.at[b, p, q])

    def swap_start(b, q):
        piece = g.at[b, core * UNITS + q]
        remote(piece, piece, d_send.at[b], d_recv.at[b, q], partner).start()

    def swap_wait(b, q):
        arrived(g.at[b, (1 - core) * UNITS + q], d_recv.at[b, q])

    def step(b, k, units=(0, UNITS)):
        def unit(q):
            if k == 0:
                scatter_start(b, 0, q)
            elif k in (1, 2):
                scatter_add(b, k - 1, q)
                scatter_start(b, k, q)
            elif k == 3:
                scatter_add(b, 2, q)
                gather_start(b, 2, q)
            elif k in (4, 5):
                gather_wait(b, 6 - k, q)
                gather_start(b, 5 - k, q)
            elif k == 6:
                gather_wait(b, 0, q)
                swap_start(b, q)
            else:
                swap_wait(b, q)
        with jax.named_scope(f'step_{b}_{k}'):
            for q in range(*units):
                unit(q)

    def token_mix(b):
        bias = jnp.concatenate([b2col[...], b2col[...]], axis=1)
        for i in range(CH // 256):
            left = g[b, 2 * i].reshape(TOK, LANES)
            right = g[b, 2 * i + 1].reshape(TOK, LANES)
            t = jnp.dot(w2t[...], jnp.concatenate([left, right], axis=1), preferred_element_type=F32)
            t = (t + bias).astype(BF16)
            cols = slice(i * 256, (i + 1) * 256)
            xv[b, :, cols] = (xv[b, :, cols].astype(F32) + t.astype(F32)).astype(BF16)

    def norm2(b):
        for i in range(ROWS // NORM_ROWS):
            rows = pl.ds(i * NORM_ROWS, NORM_ROWS)
            v[rows, :] = layer_norm(xv[b, rows, :], ln2_s[...], ln2_b[...])

    def mix(j, pieces):
        size = HID // pieces
        e = slice(j * size, (j + 1) * size)
        pre = jnp.dot(v[...], wc1[:, e], preferred_element_type=F32) + b_ch1[:, e]
        return jnp.dot(gelu(pre).astype(BF16), wc2[e, :], preferred_element_type=F32)

    small_loads[0].wait()
    small_loads[1].wait()
    loads[0].wait()
    load(2, x_hbm.at[1], xv.at[1])
    load(3, x_hbm.at[2], xv.at[2])
    load(4, x_hbm.at[3], xv.at[3])
    load(5, w_tok2_hbm.at[:, pl.ds(pl.multiple_of(me * ROWS, ROWS), ROWS)], w2raw)
    norm1(0)
    pl.semaphore_wait(barrier, 1 + 3 * (RING - 1))
    send_u(0)
    for c in small_loads[2:]:
        c.wait()
    loads[1].wait()
    for i in range(4):
        rows = pl.ds(i * 256, 256)
        w1t[:, rows] = w1raw[rows, :].T
    for m in range(4):
        row = b_tok1[m:m + 1, :]
        b1col[m * LANES:(m + 1) * LANES, :] = jnp.broadcast_to(row, (LANES, LANES)).T
    for m in range(4):
        row = b_tok2[pl.ds(me * 4 + m, 1), :]
        b2col[m * LANES:(m + 1) * LANES, :] = jnp.broadcast_to(row, (LANES, LANES)).T
    hidden(0)
    load(6, w_ch1_hbm, wc1)
    load(7, w_ch2_hbm, wc2)
    for b in range(1, IMAGES):
        loads[1 + b].wait()
        norm1(b)
        send_u(b)
    hidden(1)
    loads[5].wait()
    for i in range(2):
        cols = pl.ds(i * 256, 256)
        w2t[cols, :] = w2raw[:, cols].T
    hidden(2)
    hidden(3)
    for image, k, units in FILL:
        step(image, k, units)
    loads[6].wait()
    loads[7].wait()

    def point(b, r):
        for (image_at, point_at), todo in PLAN.items():
            if point_at == r:
                @pl.when(b == image_at)
                def _():
                    for image, k in todo:
                        step(image, k)

    def layer(b, _):
        point(b, 0)
        token_mix(b)
        norm2(b)
        acc[...] = mix(0, 4)
        point(b, 1)
        acc[...] += mix(1, 4)
        point(b, 2)
        acc[...] += mix(2, 4)
        point(b, 3)
        finish(b, mix(3, 4))
        return 0

    def finish(b, last):
        xv[b] = (xv[b].astype(F32) + (acc[...] + last + b_ch2[...])).astype(BF16)
        pltpu.make_async_copy(xv.at[b], out_hbm.at[b], store_sem.at[b]).start()

    lax.fori_loop(0, IMAGES - 1, layer, 0)
    b = IMAGES - 1
    step(b, 7)
    token_mix(b)
    norm2(b)
    acc[...] = mix(0, 2)
    finish(b, mix(1, 2))

    for b in range(IMAGES):
        arrived(upeer.at[b], u_send.at[b])
        for p, got in enumerate((got0, got1, got2)):
            arrived(got.at[b], rs_send.at[b, p])
            arrived(g.at[b, pl.ds(0, UNITS), pl.ds(0, 3 * BLOCK[p] // 8)], ag_send.at[b, p])
        arrived(g.at[b, pl.ds(0, UNITS)], d_send.at[b])
        pltpu.make_async_copy(xv.at[b], out_hbm.at[b], store_sem.at[b]).wait()


def solution(mesh):
    row_spec = P('dp', 'sp', None)
    full_spec = P()

    def local_layer(patches, ln1_scale, ln1_bias, w_tok1, b_tok1, w_tok2, b_tok2, ln2_scale, ln2_bias, w_ch1, b_ch1, w_ch2, b_ch2):
        hbm = pl.BlockSpec(memory_space=pl.ANY)
        dma = pltpu.SemaphoreType.DMA
        call = pl.pallas_call(
            layer_kernel,
            name='mixer_layer',
            out_shape=jax.ShapeDtypeStruct(patches.shape, BF16),
            in_specs=[hbm] * 13,
            out_specs=hbm,
            scratch_shapes=[
                *(pltpu.VMEM(s, F32) for s in ((1, CH), (1, CH), (TOK // LANES, LANES), (ROWS * DEVICES // LANES, LANES), (1, CH), (1, CH), (1, HID), (1, CH))),
                pltpu.VMEM((IMAGES, ROWS, CH), BF16),
                pltpu.VMEM((2 * ROWS, TOK), BF16),
                pltpu.VMEM((TOK, ROWS), BF16),
                pltpu.VMEM((TOK, 2 * ROWS), BF16),
                pltpu.VMEM((ROWS, TOK), BF16),
                pltpu.VMEM((CH, HID), BF16),
                pltpu.VMEM((HID, CH), BF16),
                pltpu.VMEM((TOK, LANES), F32),
                pltpu.VMEM((ROWS, LANES), F32),
                pltpu.VMEM((IMAGES, ROWS, CH), BF16),
                pltpu.VMEM((IMAGES, ROWS, CH // 2), BF16),
                pltpu.VMEM((IMAGES, UNITS, TOK, LANES), F32),
                pltpu.VMEM((IMAGES, UNITS, 3, BLOCK[0], LANES), F32),
                pltpu.VMEM((IMAGES, UNITS, 3, BLOCK[1], LANES), F32),
                pltpu.VMEM((IMAGES, UNITS, 3, BLOCK[2], LANES), F32),
                pltpu.VMEM((IMAGES, UNITS, BLOCK[0], LANES), F32),
                pltpu.VMEM((IMAGES, UNITS, BLOCK[1], LANES), F32),
                pltpu.VMEM((IMAGES, 2 * UNITS, TOK // 8, 8, LANES), BF16),
                pltpu.VMEM((ROWS, CH), BF16),
                pltpu.VMEM((ROWS, CH), F32),
                dma((16,)), dma((IMAGES,)),
                dma((IMAGES,)), dma((IMAGES,)),
                dma((IMAGES, 3)), dma((IMAGES, 3, UNITS)),
                dma((IMAGES, 3)), dma((IMAGES, 3, UNITS)),
                dma((IMAGES,)), dma((IMAGES, UNITS)),
            ],
            compiler_params=pltpu.CompilerParams(
                collective_id=0, has_side_effects=True, vmem_limit_bytes=64 * 1024 * 1024 - 65536),
        )
        return call(
            patches, w_tok1, w_tok2, w_ch1, w_ch2,
            ln1_scale.reshape(1, CH), ln1_bias.reshape(1, CH),
            b_tok1.reshape(TOK // LANES, LANES), b_tok2.reshape(-1, LANES),
            ln2_scale.reshape(1, CH), ln2_bias.reshape(1, CH),
            b_ch1.reshape(1, HID), b_ch2.reshape(1, CH))

    return jax.shard_map(local_layer, mesh=mesh, in_specs=(row_spec,) + (full_spec,) * 12, out_specs=row_spec, check_vma=False)
```

```python
import functools
import math

import jax
import jax.numpy as jnp
from jax import lax
from jax.experimental import pallas as pl
from jax.experimental.pallas import tpu as pltpu
from jax.sharding import PartitionSpec as P

LN_EPS = 1e-6
IMAGES = 4
ROWS = 512
CH = 1024
TOK = 512
HID = 4096
RING = 4
DEVICES = 2 * RING ** 3
LANES = 128
UNITS = CH // 2 // LANES
BLOCK = (128, 32, 8)
NORM_ROWS = 128
ALL = (0, UNITS)
FILL = (
    (0, 1, ALL), (1, 0, (0, 2)), (0, 2, ALL), (1, 0, (2, 4)), (0, 3, ALL), (1, 1, ALL), (0, 4, ALL), (1, 2, ALL),
    (0, 5, ALL), (1, 3, ALL), (0, 6, ALL), (2, 0, ALL), (0, 7, ALL),
)
PLAN = {
    (0, 1): [(1, 4), (2, 1)], (0, 2): [(1, 5), (2, 2)], (0, 3): [(2, 3), (1, 6), (3, 0)],
    (1, 0): [(1, 7), (2, 4)], (1, 1): [(2, 5), (3, 1)], (1, 2): [(3, 2)], (1, 3): [(2, 6), (3, 3)],
    (2, 0): [(2, 7), (3, 4)], (2, 1): [(3, 5)], (2, 3): [(3, 6)],
}
F32 = jnp.float32
BF16 = jnp.bfloat16

GELU_A = math.sqrt(2.0 / math.pi)
GELU_B = GELU_A * 0.044715


def gelu(a):
    return (0.5 * a) * (1.0 + jnp.tanh(a * (GELU_A + GELU_B * (a * a))))


def layer_norm(rows, scale, offset):
    wide = rows.astype(F32)
    mean = jnp.mean(wide, axis=-1, keepdims=True)
    centered = wide - mean
    var = jnp.mean(centered * centered, axis=-1, keepdims=True)
    return (centered * lax.rsqrt(var + LN_EPS) * scale + offset).astype(BF16)


def layer_kernel(
    x_hbm, w_tok1_hbm, w_tok2_hbm, w_ch1_hbm, w_ch2_hbm,
    *rest,
):
    small, (out_hbm, *rest) = rest[:8], rest[8:]
    (
    ln1_s, ln1_b, b_tok1, b_tok2, ln2_s, ln2_b, b_ch1, b_ch2,
    xv, w1raw, w2raw, w1t, w2t, wc1, wc2, b1col, b2col,
    u, upeer, part, got0, got1, got2, sum1, sum2, g, v, acc,
    load_sem, store_sem, u_send, u_recv, rs_send, rs_recv, ag_send, ag_recv, d_send, d_recv,
    ) = rest
    me = lax.axis_index('sp')
    core = me % 2
    chip = me // 2
    partner = chip * 2 + (1 - core)

    def at(index):
        return {'sp': index}

    def geometry(b, q):
        color = (q + core + b) % 3
        places, strides = [], []
        for p in range(3):
            axis = (color + p) % 3
            stride = 1 + (3 * axis * (3 * axis - 1)) // 2
            strides.append(stride)
            places.append((chip // stride) % RING)
        return places, strides

    def peer(place, stride, j):
        other = (place + j) % RING
        return other, (chip + (other - place) * stride) * 2 + core

    loads = []

    def load(n, src, dst):
        c = pltpu.make_async_copy(src, dst, load_sem.at[n])
        c.start()
        loads.append(c)

    load(0, x_hbm.at[0], xv.at[0])
    small_vmem = (ln1_s, ln1_b, b_tok1, b_tok2, ln2_s, ln2_b, b_ch1, b_ch2)
    small_loads = [pltpu.make_async_copy(s, d, load_sem.at[8 + n]) for n, (s, d) in enumerate(zip(small, small_vmem))]
    for c in small_loads:
        c.start()
    load(1, w_tok1_hbm.at[pl.ds(pl.multiple_of(chip * (2 * ROWS), 2 * ROWS), 2 * ROWS)], w1raw)

    barrier = pltpu.get_barrier_semaphore()
    pl.semaphore_signal(barrier, inc=1, device_id=at(partner), device_id_type=pl.DeviceIdType.MESH)
    for stride in (1, 4, 16):
        place = (chip // stride) % RING
        for j in range(1, RING):
            _, other = peer(place, stride, j)
            pl.semaphore_signal(barrier, inc=1, device_id=at(other), device_id_type=pl.DeviceIdType.MESH)

    def remote(src, dst, send, recv, device):
        return pltpu.make_async_remote_copy(
            src_ref=src, dst_ref=dst, send_sem=send, recv_sem=recv,
            device_id=at(device), device_id_type=pl.DeviceIdType.MESH)

    def arrived(ref, sem):
        pltpu.make_async_copy(ref, ref, sem).wait()

    half = CH // 2
    mine = pl.ds(pl.multiple_of(core * half, half), half)
    theirs = pl.ds(pl.multiple_of((1 - core) * half, half), half)

    def norm1(b):
        for i in range(ROWS // NORM_ROWS):
            rows = pl.ds(i * NORM_ROWS, NORM_ROWS)
            u[b, rows, :] = layer_norm(xv[b, rows, :], ln1_s[...], ln1_b[...])

    def send_u(b):
        remote(u.at[b, :, theirs], upeer.at[b], u_send.at[b], u_recv.at[b], partner).start()

    def hidden(b):
        arrived(upeer.at[b], u_recv.at[b])
        own = w1t[:, pl.ds(pl.multiple_of(core * ROWS, ROWS), ROWS)]
        other = w1t[:, pl.ds(pl.multiple_of((1 - core) * ROWS, ROWS), ROWS)]
        for i in range(2):
            cols = pl.ds(pl.multiple_of(core * half + i * 256, 256), 256)
            h = (jnp.dot(own, u[b, :, cols], preferred_element_type=F32)
                 + jnp.dot(other, upeer[b, :, i * 256:(i + 1) * 256], preferred_element_type=F32))
            part[b, 2 * i] = h[:, :LANES]
            part[b, 2 * i + 1] = h[:, LANES:]
            if b == 0:
                step(0, 0, (2 * i, 2 * i + 2))

    def blk(place, size):
        return pl.ds(pl.multiple_of(place * size, size), size)

    def scatter_start(b, p, q):
        src = (part, sum1, sum2)[p]
        dst = (got0, got1, got2)[p]
        places, strides = geometry(b, q)
        for j in (2, 1, 3):
            place, device = peer(places[p], strides[p], j)
            remote(src.at[b, q, blk(place, BLOCK[p])], dst.at[b, q, j - 1],
                   rs_send.at[b, p], rs_recv.at[b, p, q], device).start()

    def scatter_add(b, p, q):
        src = (part, sum1, sum2)[p]
        got = (got0, got1, got2)[p]
        places, _ = geometry(b, q)
        arrived(got.at[b, q], rs_recv.at[b, p, q])
        total = src[b, q, blk(places[p], BLOCK[p]), :] + got[b, q, 0]
        total = total + got[b, q, 1]
        total = total + got[b, q, 2]
        if p < 2:
            (sum1, sum2)[p][b, q] = total
        else:
            base = places[0] * 128 + places[1] * 32 + places[2] * 8
            h = total + b1col[blk(base // 8, 8), :]
            g[b, core * UNITS + q, base // 8] = gelu(h).astype(BF16)

    def owned(b, q, p, places):
        base = places[0] * 16
        if p >= 1:
            base = base + places[1] * 4
        if p >= 2:
            base = base + places[2]
        n = BLOCK[p] // 8
        return g.at[b, core * UNITS + q, blk(base // n, n)]

    def gather_start(b, p, q):
        places, strides = geometry(b, q)
        piece = owned(b, q, p, places)
        for j in (2, 1, 3):
            _, device = peer(places[p], strides[p], j)
            remote(piece, piece, ag_send.at[b, p], ag_recv.at[b, p, q], device).start()

    def gather_wait(b, p, q):
        arrived(g.at[b, core * UNITS + q, pl.ds(0, 3 * BLOCK[p] // 8)], ag_recv.at[b, p, q])

    def swap_start(b, q):
        piece = g.at[b, core * UNITS + q]
        remote(piece, piece, d_send.at[b], d_recv.at[b, q], partner).start()

    def swap_wait(b, q):
        arrived(g.at[b, (1 - core) * UNITS + q], d_recv.at[b, q])

    def step(b, k, units=(0, UNITS)):
        def unit(q):
            if k == 0:
                scatter_start(b, 0, q)
            elif k in (1, 2):
                scatter_add(b, k - 1, q)
                scatter_start(b, k, q)
            elif k == 3:
                scatter_add(b, 2, q)
                gather_start(b, 2, q)
            elif k in (4, 5):
                gather_wait(b, 6 - k, q)
                gather_start(b, 5 - k, q)
            elif k == 6:
                gather_wait(b, 0, q)
                swap_start(b, q)
            else:
                swap_wait(b, q)
        with jax.named_scope(f'step_{b}_{k}'):
            for q in range(*units):
                unit(q)

    def token_mix(b):
        bias = jnp.concatenate([b2col[...], b2col[...]], axis=1)
        for i in range(CH // 256):
            left = g[b, 2 * i].reshape(TOK, LANES)
            right = g[b, 2 * i + 1].reshape(TOK, LANES)
            t = jnp.dot(w2t[...], jnp.concatenate([left, right], axis=1), preferred_element_type=F32)
            t = (t + bias).astype(BF16)
            cols = slice(i * 256, (i + 1) * 256)
            xv[b, :, cols] = (xv[b, :, cols].astype(F32) + t.astype(F32)).astype(BF16)

    def norm2(b):
        for i in range(ROWS // NORM_ROWS):
            rows = pl.ds(i * NORM_ROWS, NORM_ROWS)
            v[rows, :] = layer_norm(xv[b, rows, :], ln2_s[...], ln2_b[...])

    def mix(j, pieces):
        size = HID // pieces
        e = slice(j * size, (j + 1) * size)
        pre = jnp.dot(v[...], wc1[:, e], preferred_element_type=F32) + b_ch1[:, e]
        return jnp.dot(gelu(pre).astype(BF16), wc2[e, :], preferred_element_type=F32)

    small_loads[0].wait()
    small_loads[1].wait()
    loads[0].wait()
    load(2, x_hbm.at[1], xv.at[1])
    load(3, x_hbm.at[2], xv.at[2])
    load(4, x_hbm.at[3], xv.at[3])
    load(5, w_tok2_hbm.at[:, pl.ds(pl.multiple_of(me * ROWS, ROWS), ROWS)], w2raw)
    norm1(0)
    pl.semaphore_wait(barrier, 1 + 3 * (RING - 1))
    send_u(0)
    for c in small_loads[2:]:
        c.wait()
    loads[1].wait()
    for i in range(4):
        rows = pl.ds(i * 256, 256)
        w1t[:, rows] = w1raw[rows, :].T
    for m in range(4):
        row = b_tok1[m:m + 1, :]
        b1col[m * LANES:(m + 1) * LANES, :] = jnp.broadcast_to(row, (LANES, LANES)).T
    for m in range(4):
        row = b_tok2[pl.ds(me * 4 + m, 1), :]
        b2col[m * LANES:(m + 1) * LANES, :] = jnp.broadcast_to(row, (LANES, LANES)).T
    hidden(0)
    load(6, w_ch1_hbm, wc1)
    load(7, w_ch2_hbm, wc2)
    for b in range(1, IMAGES):
        loads[1 + b].wait()
        norm1(b)
        send_u(b)
    hidden(1)
    loads[5].wait()
    for i in range(2):
        cols = pl.ds(i * 256, 256)
        w2t[cols, :] = w2raw[:, cols].T
    hidden(2)
    hidden(3)
    for image, k, units in FILL:
        step(image, k, units)
    loads[6].wait()
    loads[7].wait()

    def point(b, r):
        for (image_at, point_at), todo in PLAN.items():
            if point_at == r:
                @pl.when(b == image_at)
                def _():
                    for image, k in todo:
                        step(image, k)

    def layer(b, _):
        point(b, 0)
        token_mix(b)
        norm2(b)
        acc[...] = mix(0, 4)
        point(b, 1)
        acc[...] += mix(1, 4)
        point(b, 2)
        acc[...] += mix(2, 4)
        point(b, 3)
        finish(b, mix(3, 4))
        return 0

    def finish(b, last):
        xv[b] = (xv[b].astype(F32) + (acc[...] + last + b_ch2[...])).astype(BF16)
        pltpu.make_async_copy(xv.at[b], out_hbm.at[b], store_sem.at[b]).start()

    lax.fori_loop(0, IMAGES - 1, layer, 0)
    b = IMAGES - 1
    step(b, 7)
    token_mix(b)
    norm2(b)
    acc[...] = mix(0, 2)
    e = slice(HID // 2, HID)
    pre = jnp.dot(v[...], wc1[:, e], preferred_element_type=F32) + b_ch1[:, e]
    act = gelu(pre).astype(BF16)
    for n in range(2):
        cols = slice(n * half, (n + 1) * half)
        last = jnp.dot(act, wc2[e, cols], preferred_element_type=F32)
        xv[b, :, cols] = (xv[b, :, cols].astype(F32) + (acc[:, cols] + last + b_ch2[:, cols])).astype(BF16)
        part_of = pl.ds(n * half, half)
        pltpu.make_async_copy(xv.at[b, :, part_of], out_hbm.at[b, :, part_of], store_sem.at[b]).start()

    for b in range(IMAGES):
        arrived(upeer.at[b], u_send.at[b])
        for p, got in enumerate((got0, got1, got2)):
            arrived(got.at[b], rs_send.at[b, p])
            arrived(g.at[b, pl.ds(0, UNITS), pl.ds(0, 3 * BLOCK[p] // 8)], ag_send.at[b, p])
        arrived(g.at[b, pl.ds(0, UNITS)], d_send.at[b])
        pltpu.make_async_copy(xv.at[b], out_hbm.at[b], store_sem.at[b]).wait()


def solution(mesh):
    row_spec = P('dp', 'sp', None)
    full_spec = P()

    def local_layer(patches, ln1_scale, ln1_bias, w_tok1, b_tok1, w_tok2, b_tok2, ln2_scale, ln2_bias, w_ch1, b_ch1, w_ch2, b_ch2):
        hbm = pl.BlockSpec(memory_space=pl.ANY)
        dma = pltpu.SemaphoreType.DMA
        call = pl.pallas_call(
            layer_kernel,
            name='mixer_layer',
            out_shape=jax.ShapeDtypeStruct(patches.shape, BF16),
            in_specs=[hbm] * 13,
            out_specs=hbm,
            scratch_shapes=[
                *(pltpu.VMEM(s, F32) for s in ((1, CH), (1, CH), (TOK // LANES, LANES), (ROWS * DEVICES // LANES, LANES), (1, CH), (1, CH), (1, HID), (1, CH))),
                pltpu.VMEM((IMAGES, ROWS, CH), BF16),
                pltpu.VMEM((2 * ROWS, TOK), BF16),
                pltpu.VMEM((TOK, ROWS), BF16),
                pltpu.VMEM((TOK, 2 * ROWS), BF16),
                pltpu.VMEM((ROWS, TOK), BF16),
                pltpu.VMEM((CH, HID), BF16),
                pltpu.VMEM((HID, CH), BF16),
                pltpu.VMEM((TOK, LANES), F32),
                pltpu.VMEM((ROWS, LANES), F32),
                pltpu.VMEM((IMAGES, ROWS, CH), BF16),
                pltpu.VMEM((IMAGES, ROWS, CH // 2), BF16),
                pltpu.VMEM((IMAGES, UNITS, TOK, LANES), F32),
                pltpu.VMEM((IMAGES, UNITS, 3, BLOCK[0], LANES), F32),
                pltpu.VMEM((IMAGES, UNITS, 3, BLOCK[1], LANES), F32),
                pltpu.VMEM((IMAGES, UNITS, 3, BLOCK[2], LANES), F32),
                pltpu.VMEM((IMAGES, UNITS, BLOCK[0], LANES), F32),
                pltpu.VMEM((IMAGES, UNITS, BLOCK[1], LANES), F32),
                pltpu.VMEM((IMAGES, 2 * UNITS, TOK // 8, 8, LANES), BF16),
                pltpu.VMEM((ROWS, CH), BF16),
                pltpu.VMEM((ROWS, CH), F32),
                dma((16,)), dma((IMAGES,)),
                dma((IMAGES,)), dma((IMAGES,)),
                dma((IMAGES, 3)), dma((IMAGES, 3, UNITS)),
                dma((IMAGES, 3)), dma((IMAGES, 3, UNITS)),
                dma((IMAGES,)), dma((IMAGES, UNITS)),
            ],
            compiler_params=pltpu.CompilerParams(
                collective_id=0, has_side_effects=True, vmem_limit_bytes=64 * 1024 * 1024 - 65536),
        )
        return call(
            patches, w_tok1, w_tok2, w_ch1, w_ch2,
            ln1_scale.reshape(1, CH), ln1_bias.reshape(1, CH),
            b_tok1.reshape(TOK // LANES, LANES), b_tok2.reshape(-1, LANES),
            ln2_scale.reshape(1, CH), ln2_bias.reshape(1, CH),
            b_ch1.reshape(1, HID), b_ch2.reshape(1, CH))

    return jax.shard_map(local_layer, mesh=mesh, in_specs=(row_spec,) + (full_spec,) * 12, out_specs=row_spec, check_vma=False)
```
